32 devices in a mesh: expert: 8 (over z, x), replica: 4 (over y, core).
Axes of the slice: x: 2, y: 2, z: 4, core: 2. Of those that a mesh axis runs over, the one named last changes fastest.
Arguments:
- mantissa: bfloat16 [1048576, 128], P(('expert', 'replica')), may hold values from -4 to 4
- scales: bfloat16 [1048576], P(('expert', 'replica')), may hold values from 0.25 to 4
- counts: int32 [2048], P(('expert', 'replica')), may hold values from 256 to 512, as said below
- owner_map: int32 [1024], replicated, may hold values from 0 to 1023, each once
Outputs:
- out_mantissa: bfloat16 [32768, 128], P(('expert', 'replica'))
- out_scales: float32 [32768], P(('expert', 'replica'))
The draws below stay inside these ranges and needn't reach their ends.
Inputs may be any that keep to these rules, and one draw needn't show every extreme that they name: A device's live blocks of an expert are that expert's first counts blocks; some expert has 512 live blocks on every device, and some expert has its last block dead on every device. `owner_map`: each of 0 to 1023 appears once.
All inputs are finite; a program needn't handle non-finite values. Where the reference program divides by a largest or mean magnitude, that divisor is 1e-20 or more.
Results may differ from the reference program's by a relative error of at most 0.001.
Values may be sent and summed in bfloat16 or wider, within the bound.
A program may use at most 128 MiB of HBM per device.

```python
import math
import jax
import jax.numpy as jnp
from jax import lax

EXPERTS = 64
BLOCK = 128
GROUP = 32
BLK = 512
SOURCES = 32
NB = 32768


def draw_counts(key, part):
    gap_key = jax.random.fold_in(key, 11)
    chosen_key = jax.random.fold_in(key, 12)
    second_key = jax.random.fold_in(key, 13)
    device_key = jax.random.fold_in(key, 14)
    expert_gaps = jax.random.randint(gap_key, (EXPERTS,), 0, BLK // 2 + 1)
    chosen = jax.random.randint(chosen_key, (), 0, EXPERTS)
    second = (chosen + 1 + jax.random.randint(second_key, (), 0, EXPERTS - 1)) % EXPERTS
    expert_ids = jnp.arange(EXPERTS)
    expert_gaps = jnp.where(expert_ids == chosen, jnp.maximum(expert_gaps, 1), expert_gaps)
    expert_gaps = jnp.where(expert_ids == second, 0, expert_gaps)
    dropped = jax.random.randint(device_key, (SOURCES, EXPERTS), 0, expert_gaps[None, :] + 1)
    dropped = jnp.where((expert_ids == chosen)[None, :], jnp.maximum(dropped, 1), dropped)
    return (BLK - dropped).reshape(SOURCES * EXPERTS).astype(jnp.int32)


def steps_of(own_key, shape, split, smallest, largest):
    loudness, own = 1.0, jax.random.fold_in(own_key, 6)
    for dim, blocks in split:
        draws = jnp.exp(jax.random.uniform(jax.random.fold_in(own, dim), (blocks,), jnp.float32, smallest / len(split), largest / len(split)))
        loudness = loudness * jnp.repeat(draws, shape[dim] // blocks).reshape([-1 if axis == dim else 1 for axis in range(len(shape))])
    return loudness


def noise(stream_key, extent, spread, bound, split=(), kind=jnp.bfloat16):
    loudness = steps_of(stream_key, extent, split, -0.22, 0.18) if split else 1.0
    entries = jax.random.normal(stream_key, extent, jnp.float32) * spread * loudness
    return jnp.minimum(jnp.maximum(entries, -bound), bound).astype(kind)


def setup_inputs(seed: int = 0) -> dict:
    key_of = jax.random.split(jax.random.key(seed), 5)
    return {
        "mantissa": noise(key_of[0], (SOURCES * NB, BLOCK), 1.0, 4.0, ((0, 32),)),
        "scales": jnp.clip(jnp.exp(math.log(4.0) - 2.7725887 * jax.random.uniform(key_of[1], (SOURCES * NB,), jnp.float32) ** steps_of(key_of[1], (SOURCES * NB,), ((0, 32),), -0.2, 0.2)), 0.25, 4.0).astype(jnp.bfloat16),
        "counts": draw_counts(jax.random.fold_in(key_of[4], 71), 0),
        "owner_map": jax.random.permutation(key_of[3], NB // GROUP).astype(jnp.int32),
    }


clip_target = 0.05
epsilon = 1e-06

def reference(mantissa, scales, counts, owner_map):
    mantissas = mantissa.reshape(SOURCES, NB, BLOCK)
    scale_rows = scales.reshape(SOURCES, NB)
    load_rows = counts.reshape(SOURCES, EXPERTS)
    in_expert = (jnp.arange(NB, dtype=jnp.int32) % BLK).astype(jnp.int32)

    def accumulate(state_pair, source_item):
        summed, contributors = state_pair
        piece, source_scale, source_load = source_item
        is_live = jnp.repeat(source_load, BLK) > in_expert
        factor = jnp.where(is_live, source_scale.astype(jnp.float32), jnp.zeros((NB,), jnp.float32))
        summed = summed + piece.astype(jnp.float32) * factor[:, None]
        contributors = contributors + is_live.astype(jnp.int32)
        return ((summed, contributors), None)
    initial = (jnp.zeros((NB, BLOCK), jnp.float32), jnp.zeros((NB,), jnp.int32))
    (summed, contributors), _ = lax.scan(accumulate, initial, (mantissas, scale_rows, load_rows))
    averaged = summed / jnp.maximum(contributors, 1).astype(jnp.float32)[:, None]
    row_ids = (owner_map.astype(jnp.int32)[:, None] * GROUP + jnp.arange(GROUP, dtype=jnp.int32)[None, :]).reshape(NB).astype(jnp.int32)
    averaged = jnp.take(averaged, row_ids, axis=0)
    root_mean = jnp.sqrt(jnp.sum(averaged * averaged) / (NB * BLOCK) + epsilon)
    clip_factor = jnp.minimum(1.0, clip_target / root_mean)
    clipped = averaged * clip_factor
    block_peak = lax.optimization_barrier(jnp.max(jnp.abs(clipped), axis=1)) + epsilon
    return ((clipped / block_peak[:, None]).astype(jnp.bfloat16), block_peak)
```

```python
import functools

import jax
import jax.numpy as jnp
from jax import lax
from jax.experimental import pallas as pl
from jax.experimental.pallas import tpu as pltpu
from jax.sharding import PartitionSpec as P

GROUP = 32
LANES = 128
MESH = pl.DeviceIdType.MESH
clip_target = 0.05
epsilon = 1e-06
LOADS = 4

STREAMS = (("zxy", 2), ("xyz", 4), ("yxz", 4), ("zyx", 2), ("xyz", 3), ("yxz", 3))


def split_rows(rows):
    total = sum(share for _, share in STREAMS)
    cuts, seen = [0], 0
    for _, share in STREAMS:
        seen += share
        cuts.append((rows * seen // total) // 8 * 8)
    cuts[-1] = rows
    return cuts


def kernel(sizes, cuts, owned, live_rows, total_entries, map_ref, mant_ref, table_ref, out_ref, peak_ref,
           own, other, own_table, other_table, acc, part, parts, *rest):
    extents = dict(zip("zxy", sizes))
    n_stream = len(STREAMS)
    recv1, recv2, recv3 = rest[:n_stream], rest[n_stream:2 * n_stream], rest[2 * n_stream:3 * n_stream]
    sems = rest[3 * n_stream:6 * n_stream]
    load_sem, peer_send, peer_recv, table_sem, part_send, part_recv = rest[6 * n_stream:]
    expert, replica = lax.axis_index("expert"), lax.axis_index("replica")
    X, Y = extents["x"], extents["y"]
    n_replica = 2 * Y
    n_device = extents["z"] * X * n_replica
    me = expert * n_replica + replica
    core = replica % 2
    at = {"z": expert // X, "x": expert % X, "y": replica // 2}

    def device(pos, c):
        return (pos["z"] * X + pos["x"], pos["y"] * 2 + c)

    groups = mant_ref.shape[0]
    piece = groups // LOADS
    loads = [
        pltpu.make_async_copy(mant_ref.at[pl.ds(i * piece, piece)], own.at[pl.ds(i * piece, piece)], load_sem.at[i])
        for i in range(LOADS)
    ]
    loads.append(pltpu.make_async_copy(table_ref.at[core], own_table, load_sem.at[LOADS]))

    barrier = pltpu.get_barrier_semaphore()

    def greet(i, _):
        d = (me + i) % n_device
        pl.semaphore_signal(barrier, inc=1, device_id=(d // n_replica, d % n_replica), device_id_type=MESH)
        return 0

    lax.fori_loop(1, n_device, greet, 0)
    for c in loads:
        c.start()
    pl.semaphore_wait(barrier, n_device - 1)
    peer = device(at, 1 - core)
    swaps = [
        pltpu.make_async_remote_copy(
            src_ref=mant_ref.at[pl.ds(i * piece, piece)], dst_ref=other.at[pl.ds(i * piece, piece)],
            send_sem=peer_send.at[i], recv_sem=peer_recv.at[i], device_id=peer, device_id_type=MESH)
        for i in range(LOADS)
    ]
    swaps.append(pltpu.make_async_remote_copy(
        src_ref=table_ref.at[1 - core], dst_ref=other_table,
        send_sem=peer_send.at[LOADS], recv_sem=peer_recv.at[LOADS], device_id=peer, device_id_type=MESH))
    for c in swaps:
        c.start()
    for c in loads:
        c.wait()
    for c in swaps:
        c.wait()

    per_chunk = owned // GROUP

    def build(k, _):
        z, x, y = k // (X * Y), (k // Y) % X, k % Y
        base = (k * 2 + core) * per_chunk
        mine, theirs = own_table[k, :GROUP, :], other_table[k, :GROUP, :]
        for i in range(per_chunk):
            g = map_ref[base + i]
            value = own[g].astype(jnp.float32) * mine[:, i:i + 1]
            value += other[g].astype(jnp.float32) * theirs[:, i:i + 1]
            acc[z, x, y, i * GROUP:(i + 1) * GROUP, :] = value
        acc[z, x, y, owned:, :] = own_table[k, GROUP:, :] + other_table[k, GROUP:, :]
        return 0

    lax.fori_loop(0, sizes[0] * X * Y, build, 0)

    first, steps, finish = [], [], []

    def block(where, lo, rows, whole):
        idx = []
        for axis in "zxy":
            idx.append(slice(None) if axis in whole else where[axis])
        return acc.at[tuple(idx) + (pl.ds(lo, rows),)]

    def make_stream(s, order, lo, rows):
        a, b, c = order
        na, nb, nc = (extents[t] for t in order)

        def copy(level, up, axis, d, j=None):
            n = extents[axis]
            pos = dict(at)
            pos[axis] = jnp.clip(at[axis] + (1 if up else -1), 0, n - 1)
            where = dict(at)
            where[axis] = d
            if level == 0:
                where[b] = j
            whole = (c,) if level < 2 else ()
            slot = (0 if up else n - 1) + (d - 1 if up else d)
            dst = (recv1, recv2, recv3)[level][s]
            sem = sems[3 * s + level]
            index = (slot, j) if level == 0 else (slot,)
            return pltpu.make_async_remote_copy(
                src_ref=block(where, lo, rows, whole), dst_ref=dst.at[index],
                send_sem=sem.at[(0,) + index], recv_sem=sem.at[(1,) + index],
                device_id=device(pos, core), device_id_type=MESH), dst.at[index], block(where, lo, rows, whole)

        def send(level, up, axis, d, cond, j=None):
            @pl.when(cond)
            def _():
                copy(level, up, axis, d, j)[0].start()

            def done():
                @pl.when(cond)
                def _():
                    copy(level, up, axis, d, j)[0].wait_send()
            finish.append(done)

        def take(level, up, axis, d, cond, j=None):
            @pl.when(cond)
            def _():
                c_, got, into = copy(level, up, axis, d, j)
                c_.wait_recv()
                if level < 2:
                    for i in range(nc):
                        into[i] = into[i] + got[i]
                else:
                    into[...] = into[...] + got[...]

        def ways(axis):
            n = extents[axis]
            return [(True, d) for d in range(n - 1, 0, -1)] + [(False, d) for d in range(n - 1)]

        def edge(axis, up):
            return at[axis] == (0 if up else extents[axis] - 1)

        def initial(level, axis, j=None):
            for up, d in ways(axis):
                send(level, up, axis, d, edge(axis, up), j)

        def inner(level, axis, j=None):
            n, p = extents[axis], at[axis]
            for up, d in ways(axis):
                has = jnp.logical_and(p >= 1, d >= p) if up else jnp.logical_and(p <= n - 2, d <= p)
                take(level, up, axis, d, has, j)
                onward = jnp.logical_and(p >= 1, d > p) if up else jnp.logical_and(p <= n - 2, d < p)
                if n > 2:
                    send(level, up, axis, d, onward, j)

        t1, t2, t3 = (na - 1) * nb * nc, (nb - 1) * nc, nc - 1
        for o in range(nb - 1, -1, -1):
            j = (at[b] + o) % nb
            first.append((s, lambda j=j: initial(0, a, j)))
            steps.append((rows * t1 * (nb - o) / nb, lambda j=j: inner(0, a, j)))
        if nb == 2:
            key1 = rows * t1 * 0.5
        else:
            key1 = rows * t1
        steps.append((key1 + 0.001, lambda: initial(1, b)))
        steps.append((rows * (t1 + t2) * 1.0, lambda: (inner(1, b), initial(2, c))))
        steps.append((rows * (t1 + t2 + 2 * t3) * 1.0, lambda: inner(2, c)))

    started = {}
    for s, (order, _) in enumerate(STREAMS):
        begin = len(steps)
        make_stream(s, order, cuts[s], cuts[s + 1] - cuts[s])
        offset = started.get(order[0], 0)
        for i in range(begin, len(steps)):
            steps[i] = (steps[i][0] + offset, steps[i][1])
        na, nb, nc = (extents[t] for t in order)
        started[order[0]] = offset + (cuts[s + 1] - cuts[s]) * (na - 1) * nb * nc
    for _, run in first:
        run()
    for _, run in sorted(steps, key=lambda item: item[0]):
        run()

    mine = acc.at[at["z"], at["x"], at["y"]]
    eye = lax.broadcasted_iota(jnp.int32, (LANES, LANES), 0) == lax.broadcasted_iota(jnp.int32, (LANES, LANES), 1)
    blocks = owned // LANES
    squares = jnp.zeros((8, LANES), jnp.float32)
    for i in range(blocks):
        count = mine[owned + i:owned + i + 1, :]
        column = jnp.sum(jnp.where(eye, jnp.broadcast_to(count, (LANES, LANES)), 0.0), axis=1, keepdims=True)
        rows = pl.ds(i * LANES, LANES)
        averaged = mine[rows, :] / jnp.maximum(column, 1.0)
        mine[rows, :] = averaged
        squares += jnp.sum((averaged * averaged).reshape(LANES // 8, 8, LANES), axis=0)
    part[...] = squares

    def scalar_copy(d, sender):
        return pltpu.make_async_remote_copy(
            src_ref=part, dst_ref=parts.at[sender], send_sem=part_send.at[d], recv_sem=part_recv.at[sender],
            device_id=(d // n_replica, d % n_replica), device_id_type=MESH)

    def tell(i, _):
        scalar_copy((me + i) % n_device, me).start()
        return 0

    lax.fori_loop(1, n_device, tell, 0)
    parts[me] = squares
    for run in finish:
        run()

    def hear(i, _):
        d = (me + i) % n_device
        c = scalar_copy(d, d)
        c.wait_send()
        c.wait_recv()
        return 0

    lax.fori_loop(1, n_device, hear, 0)
    square_total = jnp.sum(jnp.sum(parts[...], axis=0), keepdims=True).reshape(1, 1)
    root_mean = jnp.sqrt(square_total / total_entries + epsilon)
    clip_factor = jnp.minimum(1.0, clip_target / root_mean)
    for i in range(blocks):
        rows = pl.ds(i * LANES, LANES)
        clipped = mine[rows, :] * clip_factor
        peak = jnp.max(jnp.abs(clipped), axis=1, keepdims=True) + epsilon
        out_ref[rows, :] = (clipped / peak).astype(jnp.bfloat16)
        peak_ref[i:i + 1, :] = jnp.sum(
            jnp.where(eye, jnp.broadcast_to(peak, (LANES, LANES)), 0.0), axis=0, keepdims=True)


def local(sizes, mantissa, scales, counts, owner_map):
    block_total, width = mantissa.shape
    experts = counts.shape[0]
    per_expert = block_total // experts
    chips = sizes[0] * sizes[1] * sizes[2]
    owned = block_total // (2 * chips)
    groups = block_total // GROUP
    per_chunk = owned // GROUP
    live_rows = -(-owned // LANES // 8) * 8
    position = jnp.arange(per_expert, dtype=jnp.int32)
    live = (counts[:, None] > position[None, :]).reshape(groups, GROUP)
    table = jnp.concatenate(
        [jnp.where(live, scales.reshape(groups, GROUP), jnp.zeros((), scales.dtype)), live.astype(scales.dtype)], axis=1)
    pick = (owner_map[:, None] == jnp.arange(groups, dtype=jnp.int32)[None, :]).astype(scales.dtype)
    placed = jnp.dot(pick, table, preferred_element_type=jnp.float32)
    by_chunk = placed.reshape(chips, 2, per_chunk, 2, GROUP)
    factor = jnp.pad(by_chunk[:, :, :, 0].transpose(1, 0, 3, 2), ((0, 0),) * 3 + ((0, LANES - per_chunk),))
    alive = by_chunk[:, :, :, 1].transpose(1, 0, 2, 3).reshape(2, chips, owned // LANES, LANES)
    alive = jnp.pad(alive, ((0, 0), (0, 0), (0, live_rows - owned // LANES), (0, 0)))
    packed = jnp.concatenate([factor, alive], axis=2)

    height = owned + live_rows
    cuts = split_rows(height)
    extents = dict(zip("zxy", sizes))
    recv1, recv2, recv3, sems = [], [], [], []
    for s, (order, _) in enumerate(STREAMS):
        rows = cuts[s + 1] - cuts[s]
        na, nb, nc = (extents[t] for t in order)
        recv1.append(pltpu.VMEM((2 * (na - 1), nb, nc, rows, width), jnp.float32))
        recv2.append(pltpu.VMEM((2 * (nb - 1), nc, rows, width), jnp.float32))
        recv3.append(pltpu.VMEM((2 * (nc - 1), rows, width), jnp.float32))
        sems.append(pltpu.SemaphoreType.DMA((2, 2 * (na - 1), nb)))
        sems.append(pltpu.SemaphoreType.DMA((2, 2 * (nb - 1))))
        sems.append(pltpu.SemaphoreType.DMA((2, 2 * (nc - 1))))
    dma = pltpu.SemaphoreType.DMA
    table_shape = packed.shape[1:]
    devices = 2 * chips
    out, peak = pl.pallas_call(
        functools.partial(kernel, sizes, cuts, owned, live_rows, float(block_total * width)),
        out_shape=(
            jax.ShapeDtypeStruct((owned, width), jnp.bfloat16),
            jax.ShapeDtypeStruct((owned // LANES, LANES), jnp.float32),
        ),
        in_specs=[
            pl.BlockSpec(memory_space=pltpu.SMEM),
            pl.BlockSpec(memory_space=pl.ANY),
            pl.BlockSpec(memory_space=pl.ANY),
        ],
        out_specs=[pl.BlockSpec(memory_space=pltpu.VMEM)] * 2,
        scratch_shapes=[
            pltpu.VMEM((groups, GROUP, width), jnp.bfloat16),
            pltpu.VMEM((groups, GROUP, width), jnp.bfloat16),
            pltpu.VMEM(table_shape, jnp.float32),
            pltpu.VMEM(table_shape, jnp.float32),
            pltpu.VMEM(tuple(sizes) + (height, width), jnp.float32),
            pltpu.VMEM((8, width), jnp.float32),
            pltpu.VMEM((devices, 8, width), jnp.float32),
            *recv1, *recv2, *recv3, *sems,
            dma((LOADS + 1,)), dma((LOADS + 1,)), dma((LOADS + 1,)), dma((1,)), dma((devices,)), dma((devices,)),
        ],
        compiler_params=pltpu.CompilerParams(
            collective_id=0, has_side_effects=True, vmem_limit_bytes=62 * 1024 * 1024),
    )(owner_map, mantissa.reshape(groups, GROUP, width), packed)
    return out, peak.reshape(owned)


def solution(mesh):
    y = mesh.shape["replica"] // 2
    x = y
    z = mesh.shape["expert"] // x
    in_specs = (
        P(("expert", "replica"), None),
        P(("expert", "replica")),
        P(("expert", "replica")),
        P(),
    )
    out_specs = (P(("expert", "replica"), None), P(("expert", "replica")))
    return jax.shard_map(functools.partial(local, (z, x, y)), mesh=mesh, in_specs=in_specs, out_specs=out_specs,
                         check_vma=False)
```

```python
import functools

import jax
import jax.numpy as jnp
from jax import lax
from jax.experimental import pallas as pl
from jax.experimental.pallas import tpu as pltpu
from jax.sharding import PartitionSpec as P

GROUP = 32
LANES = 128
MESH = pl.DeviceIdType.MESH
clip_target = 0.05
epsilon = 1e-06
LOADS = 4

STREAMS = (("zxy", 2), ("xyz", 4), ("yxz", 4), ("zyx", 2), ("xyz", 3), ("yxz", 3))


def split_rows(rows):
    total = sum(share for _, share in STREAMS)
    cuts, seen = [0], 0
    for _, share in STREAMS:
        seen += share
        cuts.append((rows * seen // total) // 8 * 8)
    cuts[-1] = rows
    return cuts


def kernel(sizes, cuts, owned, live_rows, total_entries, map_ref, mant_ref, table_ref, out_ref, peak_ref,
           own, picked, other, own_table, other_table, acc, part, parts, *rest):
    extents = dict(zip("zxy", sizes))
    n_stream = len(STREAMS)
    recv1, recv2, recv3 = rest[:n_stream], rest[n_stream:2 * n_stream], rest[2 * n_stream:3 * n_stream]
    sems = rest[3 * n_stream:6 * n_stream]
    load_sem, peer_send, peer_recv, table_sem, part_send, part_recv = rest[6 * n_stream:]
    expert, replica = lax.axis_index("expert"), lax.axis_index("replica")
    X, Y = extents["x"], extents["y"]
    n_replica = 2 * Y
    n_device = extents["z"] * X * n_replica
    me = expert * n_replica + replica
    core = replica % 2
    at = {"z": expert // X, "x": expert % X, "y": replica // 2}

    def device(pos, c):
        return (pos["z"] * X + pos["x"], pos["y"] * 2 + c)

    groups = mant_ref.shape[0]
    piece = groups // LOADS
    loads = [
        pltpu.make_async_copy(mant_ref.at[pl.ds(i * piece, piece)], own.at[pl.ds(i * piece, piece)], load_sem.at[i])
        for i in range(LOADS)
    ]
    loads.append(pltpu.make_async_copy(table_ref.at[core], own_table, load_sem.at[LOADS]))

    barrier = pltpu.get_barrier_semaphore()

    def greet(i, _):
        d = (me + i) % n_device
        pl.semaphore_signal(barrier, inc=1, device_id=(d // n_replica, d % n_replica), device_id_type=MESH)
        return 0

    lax.fori_loop(1, n_device, greet, 0)
    for c in loads:
        c.start()
    pl.semaphore_wait(barrier, n_device - 1)
    peer = device(at, 1 - core)
    table_swap = pltpu.make_async_remote_copy(
        src_ref=table_ref.at[1 - core], dst_ref=other_table,
        send_sem=table_sem.at[0], recv_sem=table_sem.at[1], device_id=peer, device_id_type=MESH)
    table_swap.start()
    for c in loads:
        c.wait()

    per_chunk = owned // GROUP
    Z = extents["z"]
    blocks_xy = [(ox, oy) for ox in range(X - 1, -1, -1) for oy in range(Y - 1, -1, -1)]

    def place(ox, oy, t):
        z, x, y = (at["z"] + t + 1) % Z, (at["x"] + ox) % X, (at["y"] + oy) % Y
        return z, x, y, (z * X + x) * Y + y

    def swap(k):
        return pltpu.make_async_remote_copy(
            src_ref=picked.at[k], dst_ref=other.at[k], send_sem=peer_send.at[k], recv_sem=peer_recv.at[k],
            device_id=peer, device_id_type=MESH)

    def gather(ox, oy):
        def one(t, _):
            k = place(ox, oy, t)[3]
            base = (k * 2 + 1 - core) * per_chunk
            for i in range(per_chunk):
                picked[k, i] = own[map_ref[base + i]]
            swap(k).start()
            return 0
        lax.fori_loop(0, Z, one, 0)

    def build(ox, oy):
        def one(t, _):
            z, x, y, k = place(ox, oy, t)
            swap(k).wait_recv()
            base = (k * 2 + core) * per_chunk
            mine, theirs = own_table[k, :GROUP, :], other_table[k, :GROUP, :]
            for i in range(per_chunk):
                value = own[map_ref[base + i]].astype(jnp.float32) * mine[:, i:i + 1]
                value += other[k, i].astype(jnp.float32) * theirs[:, i:i + 1]
                acc[z, x, y, i * GROUP:(i + 1) * GROUP, :] = value
            acc[z, x, y, owned:, :] = own_table[k, GROUP:, :] + other_table[k, GROUP:, :]
            return 0
        lax.fori_loop(0, Z, one, 0)

    for ox, oy in blocks_xy:
        gather(ox, oy)
    table_swap.wait()

    first, steps, finish = [], [], []

    def block(where, lo, rows, whole):
        idx = []
        for axis in "zxy":
            idx.append(slice(None) if axis in whole else where[axis])
        return acc.at[tuple(idx) + (pl.ds(lo, rows),)]

    def make_stream(s, order, lo, rows):
        a, b, c = order
        na, nb, nc = (extents[t] for t in order)

        def copy(level, away, axis, d, j=None):
            n = extents[axis]
            turned = (2 * at[axis]) // n
            up = away * (1 - turned) + (1 - away) * turned
            real = d * (1 - turned) + (n - 1 - d) * turned
            pos = dict(at)
            pos[axis] = (at[axis] + 2 * up - 1 + n) % n
            where = dict(at)
            where[axis] = real
            if level == 0:
                where[b] = j
            whole = (c,) if level < 2 else ()
            slot = up * (real - 1) + (1 - up) * (n - 1 + real)
            dst = (recv1, recv2, recv3)[level][s]
            sem = sems[3 * s + level]
            index = (slot, j) if level == 0 else (slot,)
            return pltpu.make_async_remote_copy(
                src_ref=block(where, lo, rows, whole), dst_ref=dst.at[index],
                send_sem=sem.at[(0,) + index], recv_sem=sem.at[(1,) + index],
                device_id=device(pos, core), device_id_type=MESH), dst.at[index], block(where, lo, rows, whole)

        def when(cond, run):
            if cond is True:
                run()
            elif cond is not False:
                pl.when(cond)(run)

        def send(level, away, axis, d, cond, j=None):
            when(cond, lambda: copy(level, away, axis, d, j)[0].start())
            finish.append(lambda: when(cond, lambda: copy(level, away, axis, d, j)[0].wait_send()))

        def take(level, away, axis, d, cond, j=None):
            def run():
                c_, got, into = copy(level, away, axis, d, j)
                c_.wait_recv()
                if level < 2:
                    for i in range(nc):
                        into[i] = into[i] + got[i]
                else:
                    into[...] = into[...] + got[...]
            when(cond, run)

        def near(axis):
            n, p = extents[axis], at[axis]
            turned = (2 * p) // n
            return p * (1 - turned) + (n - 1 - p) * turned

        def initial(level, axis, j=None):
            n = extents[axis]
            for d in range(n - 1, 0, -1):
                send(level, 1, axis, d, True if n == 2 else near(axis) == 0, j)

        def inner(level, axis, j=None):
            n = extents[axis]
            half = n // 2
            if n == 2:
                take(level, 0, axis, 0, True, j)
                return
            p = near(axis)
            for i in range(n - 1):
                up_d, down_d = n - 1 - i, i
                take(level, 1, axis, up_d, jnp.logical_and(p >= 1, p <= up_d), j)
                if up_d > 1:
                    send(level, 1, axis, up_d, jnp.logical_and(p >= 1, p < up_d), j)
                if down_d < half:
                    take(level, 0, axis, down_d, p >= down_d, j)
                    if down_d < half - 1:
                        send(level, 0, axis, down_d, p > down_d, j)

        t1, t2, t3 = (na - 1) * nb * nc, (nb - 1) * nc, nc - 1
        for o in range(nb - 1, -1, -1):
            j = (at[b] + o) % nb
            spans = {a: range(1, na), b: (o,), c: range(nc)}
            needs = [(ox, oy) for ox in spans["x"] for oy in spans["y"]]
            ready = max(blocks_xy.index(n) for n in needs)
            first.append((ready, lambda j=j: initial(0, a, j)))
            steps.append((rows * t1 * (nb - o) / nb, lambda j=j: inner(0, a, j)))
        if nb == 2:
            key1 = rows * t1 * 0.5
        else:
            key1 = rows * t1
        steps.append((key1 + 0.001, lambda: initial(1, b)))
        steps.append((rows * (t1 + t2) * 1.0, lambda: (inner(1, b), initial(2, c))))
        steps.append((rows * (t1 + t2 + 2 * t3) * 1.0, lambda: inner(2, c)))

    started = {}
    for s, (order, _) in enumerate(STREAMS):
        begin = len(steps)
        make_stream(s, order, cuts[s], cuts[s + 1] - cuts[s])
        offset = started.get(order[0], 0)
        for i in range(begin, len(steps)):
            steps[i] = (steps[i][0] + offset, steps[i][1])
        na, nb, nc = (extents[t] for t in order)
        started[order[0]] = offset + (cuts[s + 1] - cuts[s]) * (na - 1) * nb * nc
    for at_block, (ox, oy) in enumerate(blocks_xy):
        build(ox, oy)
        for ready, run in first:
            if ready == at_block:
                run()
    for _, run in sorted(steps, key=lambda item: item[0]):
        run()

    mine = acc.at[at["z"], at["x"], at["y"]]
    eye = lax.broadcasted_iota(jnp.int32, (LANES, LANES), 0) == lax.broadcasted_iota(jnp.int32, (LANES, LANES), 1)
    blocks = owned // LANES
    squares = jnp.zeros((8, LANES), jnp.float32)
    for i in range(blocks):
        count = mine[owned + i:owned + i + 1, :]
        column = jnp.sum(jnp.where(eye, jnp.broadcast_to(count, (LANES, LANES)), 0.0), axis=1, keepdims=True)
        rows = pl.ds(i * LANES, LANES)
        averaged = mine[rows, :] / jnp.maximum(column, 1.0)
        mine[rows, :] = averaged
        squares += jnp.sum((averaged * averaged).reshape(LANES // 8, 8, LANES), axis=0)
    part[...] = squares

    def scalar_copy(d, sender):
        return pltpu.make_async_remote_copy(
            src_ref=part, dst_ref=parts.at[sender], send_sem=part_send.at[d], recv_sem=part_recv.at[sender],
            device_id=(d // n_replica, d % n_replica), device_id_type=MESH)

    def tell(i, _):
        scalar_copy((me + i) % n_device, me).start()
        return 0

    lax.fori_loop(1, n_device, tell, 0)
    parts[me] = squares
    for run in finish:
        run()
    for k in range(sizes[0] * X * Y):
        swap(k).wait_send()

    def hear(i, _):
        d = (me + i) % n_device
        c = scalar_copy(d, d)
        c.wait_send()
        c.wait_recv()
        return 0

    lax.fori_loop(1, n_device, hear, 0)
    square_total = jnp.sum(jnp.sum(parts[...], axis=0), keepdims=True).reshape(1, 1)
    root_mean = jnp.sqrt(square_total / total_entries + epsilon)
    clip_factor = jnp.minimum(1.0, clip_target / root_mean)
    for i in range(blocks):
        rows = pl.ds(i * LANES, LANES)
        clipped = mine[rows, :] * clip_factor
        peak = jnp.max(jnp.abs(clipped), axis=1, keepdims=True) + epsilon
        out_ref[rows, :] = (clipped / peak).astype(jnp.bfloat16)
        peak_ref[i:i + 1, :] = jnp.sum(
            jnp.where(eye, jnp.broadcast_to(peak, (LANES, LANES)), 0.0), axis=0, keepdims=True)


def local(sizes, mantissa, scales, counts, owner_map):
    block_total, width = mantissa.shape
    experts = counts.shape[0]
    per_expert = block_total // experts
    chips = sizes[0] * sizes[1] * sizes[2]
    owned = block_total // (2 * chips)
    groups = block_total // GROUP
    per_chunk = owned // GROUP
    live_rows = -(-owned // LANES // 8) * 8
    position = jnp.arange(per_expert, dtype=jnp.int32)
    live = (counts[:, None] > position[None, :]).reshape(groups, GROUP)
    table = jnp.concatenate(
        [jnp.where(live, scales.reshape(groups, GROUP), jnp.zeros((), scales.dtype)), live.astype(scales.dtype)], axis=1)
    pick = (owner_map[:, None] == jnp.arange(groups, dtype=jnp.int32)[None, :]).astype(scales.dtype)
    placed = jnp.dot(pick, table, preferred_element_type=jnp.float32)
    by_chunk = placed.reshape(chips, 2, per_chunk, 2, GROUP)
    factor = jnp.pad(by_chunk[:, :, :, 0].transpose(1, 0, 3, 2), ((0, 0),) * 3 + ((0, LANES - per_chunk),))
    alive = by_chunk[:, :, :, 1].transpose(1, 0, 2, 3).reshape(2, chips, owned // LANES, LANES)
    alive = jnp.pad(alive, ((0, 0), (0, 0), (0, live_rows - owned // LANES), (0, 0)))
    packed = jnp.concatenate([factor, alive], axis=2)

    height = owned + live_rows
    cuts = split_rows(height)
    extents = dict(zip("zxy", sizes))
    recv1, recv2, recv3, sems = [], [], [], []
    for s, (order, _) in enumerate(STREAMS):
        rows = cuts[s + 1] - cuts[s]
        na, nb, nc = (extents[t] for t in order)
        recv1.append(pltpu.VMEM((2 * (na - 1), nb, nc, rows, width), jnp.float32))
        recv2.append(pltpu.VMEM((2 * (nb - 1), nc, rows, width), jnp.float32))
        recv3.append(pltpu.VMEM((2 * (nc - 1), rows, width), jnp.float32))
        sems.append(pltpu.SemaphoreType.DMA((2, 2 * (na - 1), nb)))
        sems.append(pltpu.SemaphoreType.DMA((2, 2 * (nb - 1))))
        sems.append(pltpu.SemaphoreType.DMA((2, 2 * (nc - 1))))
    dma = pltpu.SemaphoreType.DMA
    table_shape = packed.shape[1:]
    devices = 2 * chips
    out, peak = pl.pallas_call(
        functools.partial(kernel, sizes, cuts, owned, live_rows, float(block_total * width)),
        out_shape=(
            jax.ShapeDtypeStruct((owned, width), jnp.bfloat16),
            jax.ShapeDtypeStruct((owned // LANES, LANES), jnp.float32),
        ),
        in_specs=[
            pl.BlockSpec(memory_space=pltpu.SMEM),
            pl.BlockSpec(memory_space=pl.ANY),
            pl.BlockSpec(memory_space=pl.ANY),
        ],
        out_specs=[pl.BlockSpec(memory_space=pltpu.VMEM)] * 2,
        scratch_shapes=[
            pltpu.VMEM((groups, GROUP, width), jnp.bfloat16),
            pltpu.VMEM((chips, per_chunk, GROUP, width), jnp.bfloat16),
            pltpu.VMEM((chips, per_chunk, GROUP, width), jnp.bfloat16),
            pltpu.VMEM(table_shape, jnp.float32),
            pltpu.VMEM(table_shape, jnp.float32),
            pltpu.VMEM(tuple(sizes) + (height, width), jnp.float32),
            pltpu.VMEM((8, width), jnp.float32),
            pltpu.VMEM((devices, 8, width), jnp.float32),
            *recv1, *recv2, *recv3, *sems,
            dma((LOADS + 1,)), dma((chips,)), dma((chips,)), dma((2,)), dma((devices,)), dma((devices,)),
        ],
        compiler_params=pltpu.CompilerParams(
            collective_id=0, has_side_effects=True, vmem_limit_bytes=62 * 1024 * 1024),
    )(owner_map, mantissa.reshape(groups, GROUP, width), packed)
    return out, peak.reshape(owned)


def solution(mesh):
    y = mesh.shape["replica"] // 2
    x = y
    z = mesh.shape["expert"] // x
    in_specs = (
        P(("expert", "replica"), None),
        P(("expert", "replica")),
        P(("expert", "replica")),
        P(),
    )
    out_specs = (P(("expert", "replica"), None), P(("expert", "replica")))
    return jax.shard_map(functools.partial(local, (z, x, y)), mesh=mesh, in_specs=in_specs, out_specs=out_specs,
                         check_vma=False)
```

```python
import functools
import heapq

import jax
import jax.numpy as jnp
from jax import lax
from jax.experimental import pallas as pl
from jax.experimental.pallas import tpu as pltpu
from jax.sharding import PartitionSpec as P

GROUP = 32
LANES = 128
MESH = pl.DeviceIdType.MESH
clip_target = 0.05
epsilon = 1e-06
LOADS = 4

STREAMS = (("zxy", 2), ("xyz", 4), ("yxz", 4), ("zyx", 2), ("xyz", 3), ("yxz", 3))


def split_rows(rows):
    total = sum(share for _, share in STREAMS)
    cuts, seen = [0], 0
    for _, share in STREAMS:
        seen += share
        cuts.append((rows * seen // total) // 8 * 8)
    cuts[-1] = rows
    return cuts


def plan(extents, cuts):
    link, events, keys, ends = dict.fromkeys(extents, 0.0), [], {}, {}
    for s, (order, _) in enumerate(STREAMS):
        (a, b, c), rows = order, cuts[s + 1] - cuts[s]
        for o in range(extents[b] - 1, -1, -1):
            link[a] += rows * (extents[a] - 1) * extents[c]
            heapq.heappush(events, (link[a], s, 0, o))
            ends[s] = link[a]
    while events:
        t, s, level, o = heapq.heappop(events)
        (a, b, c), rows = STREAMS[s][0], cuts[s + 1] - cuts[s]
        if level == 1:
            t = max(t, ends[s])
        keys[s, level, o] = t
        if level == 0 and o == (1 if extents[b] == 2 else 0):
            link[b] = max(t, link[b]) + rows * (extents[b] - 1) * extents[c]
            heapq.heappush(events, (link[b], s, 1, 0))
        if level == 1:
            link[c] = max(t, link[c]) + rows * (extents[c] - 1)
            heapq.heappush(events, (link[c], s, 2, 0))
    return keys


def kernel(sizes, cuts, owned, live_rows, total_entries, map_ref, mant_ref, table_ref, out_ref, peak_ref,
           own, picked, other, own_table, other_table, acc, part, parts, *rest):
    extents = dict(zip("zxy", sizes))
    n_stream = len(STREAMS)
    recv1, recv2, recv3 = rest[:n_stream], rest[n_stream:2 * n_stream], rest[2 * n_stream:3 * n_stream]
    sems = rest[3 * n_stream:6 * n_stream]
    load_sem, peer_send, peer_recv, table_sem, part_send, part_recv = rest[6 * n_stream:]
    expert, replica = lax.axis_index("expert"), lax.axis_index("replica")
    X, Y = extents["x"], extents["y"]
    n_replica = 2 * Y
    n_device = extents["z"] * X * n_replica
    me = expert * n_replica + replica
    core = replica % 2
    at = {"z": expert // X, "x": expert % X, "y": replica // 2}

    def device(pos, c):
        return (pos["z"] * X + pos["x"], pos["y"] * 2 + c)

    groups = mant_ref.shape[0]
    piece = groups // LOADS
    loads = [
        pltpu.make_async_copy(mant_ref.at[pl.ds(i * piece, piece)], own.at[pl.ds(i * piece, piece)], load_sem.at[i])
        for i in range(LOADS)
    ]
    loads.append(pltpu.make_async_copy(table_ref.at[core], own_table, load_sem.at[LOADS]))

    barrier = pltpu.get_barrier_semaphore()

    def greet(i, _):
        d = (me + i) % n_device
        pl.semaphore_signal(barrier, inc=1, device_id=(d // n_replica, d % n_replica), device_id_type=MESH)
        return 0

    lax.fori_loop(1, n_device, greet, 0)
    for c in loads:
        c.start()
    pl.semaphore_wait(barrier, n_device - 1)
    peer = device(at, 1 - core)
    table_swap = pltpu.make_async_remote_copy(
        src_ref=table_ref.at[1 - core], dst_ref=other_table,
        send_sem=table_sem.at[0], recv_sem=table_sem.at[1], device_id=peer, device_id_type=MESH)
    table_swap.start()
    for c in loads:
        c.wait()

    per_chunk = owned // GROUP
    Z = extents["z"]
    blocks_xy = [(ox, oy) for ox in range(X - 1, -1, -1) for oy in range(Y - 1, -1, -1)]

    def place(ox, oy, t):
        z, x, y = (at["z"] + t + 1) % Z, (at["x"] + ox) % X, (at["y"] + oy) % Y
        return z, x, y, (z * X + x) * Y + y

    def swap(k):
        return pltpu.make_async_remote_copy(
            src_ref=picked.at[k], dst_ref=other.at[k], send_sem=peer_send.at[k], recv_sem=peer_recv.at[k],
            device_id=peer, device_id_type=MESH)

    def gather(ox, oy):
        def one(t, _):
            k = place(ox, oy, t)[3]
            base = (k * 2 + 1 - core) * per_chunk
            for i in range(per_chunk):
                picked[k, i] = own[map_ref[base + i]]
            swap(k).start()
            return 0
        lax.fori_loop(0, Z, one, 0)

    def build(ox, oy):
        def one(t, _):
            z, x, y, k = place(ox, oy, t)
            swap(k).wait_recv()
            base = (k * 2 + core) * per_chunk
            mine, theirs = own_table[k, :GROUP, :], other_table[k, :GROUP, :]
            for i in range(per_chunk):
                value = own[map_ref[base + i]].astype(jnp.float32) * mine[:, i:i + 1]
                value += other[k, i].astype(jnp.float32) * theirs[:, i:i + 1]
                acc[z, x, y, i * GROUP:(i + 1) * GROUP, :] = value
            acc[z, x, y, owned:, :] = own_table[k, GROUP:, :] + other_table[k, GROUP:, :]
            return 0
        lax.fori_loop(0, Z, one, 0)

    for ox, oy in blocks_xy:
        gather(ox, oy)
    table_swap.wait()

    first, steps, finish = [], [], []

    def block(where, lo, rows, whole):
        idx = []
        for axis in "zxy":
            idx.append(slice(None) if axis in whole else where[axis])
        return acc.at[tuple(idx) + (pl.ds(lo, rows),)]

    def make_stream(s, order, lo, rows):
        a, b, c = order
        na, nb, nc = (extents[t] for t in order)

        def copy(level, away, axis, d, j=None):
            n = extents[axis]
            turned = (2 * at[axis]) // n
            up = away * (1 - turned) + (1 - away) * turned
            real = d * (1 - turned) + (n - 1 - d) * turned
            pos = dict(at)
            pos[axis] = (at[axis] + 2 * up - 1 + n) % n
            where = dict(at)
            where[axis] = real
            if level == 0:
                where[b] = j
            whole = (c,) if level < 2 else ()
            slot = up * (real - 1) + (1 - up) * (n - 1 + real)
            dst = (recv1, recv2, recv3)[level][s]
            sem = sems[3 * s + level]
            index = (slot, j) if level == 0 else (slot,)
            return pltpu.make_async_remote_copy(
                src_ref=block(where, lo, rows, whole), dst_ref=dst.at[index],
                send_sem=sem.at[(0,) + index], recv_sem=sem.at[(1,) + index],
                device_id=device(pos, core), device_id_type=MESH), dst.at[index], block(where, lo, rows, whole)

        def when(cond, run):
            if cond is True:
                run()
            elif cond is not False:
                pl.when(cond)(run)

        def send(level, away, axis, d, cond, j=None):
            when(cond, lambda: copy(level, away, axis, d, j)[0].start())
            finish.append(lambda: when(cond, lambda: copy(level, away, axis, d, j)[0].wait_send()))

        def take(level, away, axis, d, cond, j=None):
            def run():
                c_, got, into = copy(level, away, axis, d, j)
                c_.wait_recv()
                if level < 2:
                    for i in range(nc):
                        into[i] = into[i] + got[i]
                else:
                    into[...] = into[...] + got[...]
            when(cond, run)

        def near(axis):
            n, p = extents[axis], at[axis]
            turned = (2 * p) // n
            return p * (1 - turned) + (n - 1 - p) * turned

        def initial(level, axis, j=None):
            n = extents[axis]
            for d in range(n - 1, 0, -1):
                send(level, 1, axis, d, True if n == 2 else near(axis) == 0, j)

        def inner(level, axis, j=None):
            n = extents[axis]
            half = n // 2
            if n == 2:
                take(level, 0, axis, 0, True, j)
                return
            p = near(axis)
            for i in range(n - 1):
                up_d, down_d = n - 1 - i, i
                take(level, 1, axis, up_d, jnp.logical_and(p >= 1, p <= up_d), j)
                if up_d > 1:
                    send(level, 1, axis, up_d, jnp.logical_and(p >= 1, p < up_d), j)
                if down_d < half:
                    take(level, 0, axis, down_d, p >= down_d, j)
                    if down_d < half - 1:
                        send(level, 0, axis, down_d, p > down_d, j)

        for o in range(nb - 1, -1, -1):
            j = (at[b] + o) % nb
            spans = {a: range(1, na), b: (o,), c: range(nc)}
            needs = [(ox, oy) for ox in spans["x"] for oy in spans["y"]]
            ready = max(blocks_xy.index(n) for n in needs)
            first.append((ready, lambda j=j: initial(0, a, j)))
            steps.append(((keys[s, 0, o], 0, len(steps)), lambda j=j: inner(0, a, j)))
            if o == (1 if nb == 2 else 0):
                steps.append(((keys[s, 0, o], 0, len(steps)), lambda: initial(1, b)))
        steps.append(((keys[s, 1, 0], 1, len(steps)), lambda: (inner(1, b), initial(2, c))))
        steps.append(((keys[s, 2, 0], 2, len(steps)), lambda: inner(2, c)))

    keys = plan(extents, cuts)
    for s, (order, _) in enumerate(STREAMS):
        make_stream(s, order, cuts[s], cuts[s + 1] - cuts[s])
    for at_block, (ox, oy) in enumerate(blocks_xy):
        build(ox, oy)
        for ready, run in first:
            if ready == at_block:
                run()
    for _, run in sorted(steps, key=lambda item: item[0]):
        run()

    mine = acc.at[at["z"], at["x"], at["y"]]
    eye = lax.broadcasted_iota(jnp.int32, (LANES, LANES), 0) == lax.broadcasted_iota(jnp.int32, (LANES, LANES), 1)
    blocks = owned // LANES
    squares = jnp.zeros((8, LANES), jnp.float32)
    for i in range(blocks):
        count = mine[owned + i:owned + i + 1, :]
        column = jnp.sum(jnp.where(eye, jnp.broadcast_to(count, (LANES, LANES)), 0.0), axis=1, keepdims=True)
        rows = pl.ds(i * LANES, LANES)
        averaged = mine[rows, :] / jnp.maximum(column, 1.0)
        mine[rows, :] = averaged
        squares += jnp.sum((averaged * averaged).reshape(LANES // 8, 8, LANES), axis=0)
    part[...] = squares

    def scalar_copy(d, sender):
        return pltpu.make_async_remote_copy(
            src_ref=part, dst_ref=parts.at[sender], send_sem=part_send.at[d], recv_sem=part_recv.at[sender],
            device_id=(d // n_replica, d % n_replica), device_id_type=MESH)

    def tell(i, _):
        scalar_copy((me + i) % n_device, me).start()
        return 0

    lax.fori_loop(1, n_device, tell, 0)
    parts[me] = squares
    for run in finish:
        run()
    for k in range(sizes[0] * X * Y):
        swap(k).wait_send()

    def hear(i, _):
        d = (me + i) % n_device
        c = scalar_copy(d, d)
        c.wait_send()
        c.wait_recv()
        return 0

    lax.fori_loop(1, n_device, hear, 0)
    square_total = jnp.sum(jnp.sum(parts[...], axis=0), keepdims=True).reshape(1, 1)
    root_mean = jnp.sqrt(square_total / total_entries + epsilon)
    clip_factor = jnp.minimum(1.0, clip_target / root_mean)
    for i in range(blocks):
        rows = pl.ds(i * LANES, LANES)
        clipped = mine[rows, :] * clip_factor
        peak = jnp.max(jnp.abs(clipped), axis=1, keepdims=True) + epsilon
        out_ref[rows, :] = (clipped / peak).astype(jnp.bfloat16)
        peak_ref[i:i + 1, :] = jnp.sum(
            jnp.where(eye, jnp.broadcast_to(peak, (LANES, LANES)), 0.0), axis=0, keepdims=True)


def local(sizes, mantissa, scales, counts, owner_map):
    block_total, width = mantissa.shape
    experts = counts.shape[0]
    per_expert = block_total // experts
    chips = sizes[0] * sizes[1] * sizes[2]
    owned = block_total // (2 * chips)
    groups = block_total // GROUP
    per_chunk = owned // GROUP
    live_rows = -(-owned // LANES // 8) * 8
    position = jnp.arange(per_expert, dtype=jnp.int32)
    live = (counts[:, None] > position[None, :]).reshape(groups, GROUP)
    table = jnp.concatenate(
        [jnp.where(live, scales.reshape(groups, GROUP), jnp.zeros((), scales.dtype)), live.astype(scales.dtype)], axis=1)
    pick = (owner_map[:, None] == jnp.arange(groups, dtype=jnp.int32)[None, :]).astype(scales.dtype)
    placed = jnp.dot(pick, table, preferred_element_type=jnp.float32)
    by_chunk = placed.reshape(chips, 2, per_chunk, 2, GROUP)
    factor = jnp.pad(by_chunk[:, :, :, 0].transpose(1, 0, 3, 2), ((0, 0),) * 3 + ((0, LANES - per_chunk),))
    alive = by_chunk[:, :, :, 1].transpose(1, 0, 2, 3).reshape(2, chips, owned // LANES, LANES)
    alive = jnp.pad(alive, ((0, 0), (0, 0), (0, live_rows - owned // LANES), (0, 0)))
    packed = jnp.concatenate([factor, alive], axis=2)

    height = owned + live_rows
    cuts = split_rows(height)
    extents = dict(zip("zxy", sizes))
    recv1, recv2, recv3, sems = [], [], [], []
    for s, (order, _) in enumerate(STREAMS):
        rows = cuts[s + 1] - cuts[s]
        na, nb, nc = (extents[t] for t in order)
        recv1.append(pltpu.VMEM((2 * (na - 1), nb, nc, rows, width), jnp.float32))
        recv2.append(pltpu.VMEM((2 * (nb - 1), nc, rows, width), jnp.float32))
        recv3.append(pltpu.VMEM((2 * (nc - 1), rows, width), jnp.float32))
        sems.append(pltpu.SemaphoreType.DMA((2, 2 * (na - 1), nb)))
        sems.append(pltpu.SemaphoreType.DMA((2, 2 * (nb - 1))))
        sems.append(pltpu.SemaphoreType.DMA((2, 2 * (nc - 1))))
    dma = pltpu.SemaphoreType.DMA
    table_shape = packed.shape[1:]
    devices = 2 * chips
    out, peak = pl.pallas_call(
        functools.partial(kernel, sizes, cuts, owned, live_rows, float(block_total * width)),
        out_shape=(
            jax.ShapeDtypeStruct((owned, width), jnp.bfloat16),
            jax.ShapeDtypeStruct((owned // LANES, LANES), jnp.float32),
        ),
        in_specs=[
            pl.BlockSpec(memory_space=pltpu.SMEM),
            pl.BlockSpec(memory_space=pl.ANY),
            pl.BlockSpec(memory_space=pl.ANY),
        ],
        out_specs=[pl.BlockSpec(memory_space=pltpu.VMEM)] * 2,
        scratch_shapes=[
            pltpu.VMEM((groups, GROUP, width), jnp.bfloat16),
            pltpu.VMEM((chips, per_chunk, GROUP, width), jnp.bfloat16),
            pltpu.VMEM((chips, per_chunk, GROUP, width), jnp.bfloat16),
            pltpu.VMEM(table_shape, jnp.float32),
            pltpu.VMEM(table_shape, jnp.float32),
            pltpu.VMEM(tuple(sizes) + (height, width), jnp.float32),
            pltpu.VMEM((8, width), jnp.float32),
            pltpu.VMEM((devices, 8, width), jnp.float32),
            *recv1, *recv2, *recv3, *sems,
            dma((LOADS + 1,)), dma((chips,)), dma((chips,)), dma((2,)), dma((devices,)), dma((devices,)),
        ],
        compiler_params=pltpu.CompilerParams(
            collective_id=0, has_side_effects=True, vmem_limit_bytes=62 * 1024 * 1024),
    )(owner_map, mantissa.reshape(groups, GROUP, width), packed)
    return out, peak.reshape(owned)


def solution(mesh):
    y = mesh.shape["replica"] // 2
    x = y
    z = mesh.shape["expert"] // x
    in_specs = (
        P(("expert", "replica"), None),
        P(("expert", "replica")),
        P(("expert", "replica")),
        P(),
    )
    out_specs = (P(("expert", "replica"), None), P(("expert", "replica")))
    return jax.shard_map(functools.partial(local, (z, x, y)), mesh=mesh, in_specs=in_specs, out_specs=out_specs,
                         check_vma=False)
```
